32 devices in a mesh: tile: 8 (over z, x), sub: 4 (over y, core).
Axes of the slice: x: 2, y: 2, z: 4, core: 2. Of those that a mesh axis runs over, the one named last changes fastest.
Arguments:
- initial_state: float32 [8, 64, 1024], P('tile', None, 'sub'), may hold values from -6 to 6
- cotangent: float32 [8, 64, 1024], P('tile', None, 'sub'), may hold values from -6 to 6
- w_in: bfloat16 [576, 1024], replicated, may hold values from -0.25 to 0.25
- b_in: float32 [1024], replicated, may hold values from -3 to 3
- w_out: bfloat16 [64, 1024], replicated, may hold values from -0.1875 to 0.1875
- edge_flips: int32 [8, 2], P('tile'), may hold values 0 or 1
Outputs:
- final_state: float32 [8, 64, 1024], P('tile', None, 'sub')
- grad_state: float32 [8, 64, 1024], P('tile', None, 'sub')
- grad_w_in: float32 [576, 1024], replicated
- grad_b_in: float32 [1024], replicated
- grad_w_out: float32 [64, 1024], replicated
The draws below stay inside these ranges and needn't reach their ends.
All inputs are finite; a program needn't handle non-finite values. No bound on the sum of `edge_flips` on one device may be relied on, other than what follows from the above.
Results may differ from the reference program's by a relative error of at most 0.006.
Values may be sent and summed in bfloat16 or wider, within the bound.
A program may use at most 64 MiB of HBM per device.

```python
import jax
import jax.numpy as jnp

LEVELS = 64
HIDDEN_SIZE = 1024
IN_WIDTH = 576
STEPS = 4
TILE_ROW = 4
SIDE = 32
COLS = 1024
TILES = 8


def set_ends(values, rng, low, high):
    shape = values.shape
    place = [jax.random.randint(jax.random.fold_in(rng, axis), (), 0, shape[axis]) for axis in range(len(shape))]
    values = values.at[tuple(place)].set(low)
    longest = shape.index(max(shape))
    place[longest] = (place[longest] + 1) % shape[longest]
    return values.at[tuple(place)].set(high)


def block_levels(stream_key, dims, split, least, largest):
    level, own = 1.0, jax.random.fold_in(stream_key, 6)
    for dim, shards_of in split:
        steps = jnp.exp(jax.random.uniform(jax.random.fold_in(own, dim), (shards_of,), jnp.float32, least / len(split), largest / len(split)))
        level = level * jnp.repeat(steps, dims[dim] // shards_of).reshape([-1 if axis == dim else 1 for axis in range(len(dims))])
    return level


def bell_draw(own_key, extent, deviation, bound, cuts=(), dtype=jnp.bfloat16):
    drawn = deviation * jax.random.normal(own_key, extent, jnp.float32)
    if cuts:
        drawn = drawn * block_levels(own_key, extent, cuts, -0.22, 0.18)
    return jnp.clip(drawn, -bound, bound).astype(dtype)


def setup_inputs(seed: int = 0) -> dict:
    key_list = jax.random.split(jax.random.key(seed), 7)
    return {
        "initial_state": bell_draw(key_list[0], (TILES, LEVELS, COLS), 1.0, 6.0, ((0, 8), (2, 4)), jnp.float32),
        "cotangent": bell_draw(key_list[1], (TILES, LEVELS, COLS), 1.0, 6.0, ((0, 8), (2, 4)), jnp.float32),
        "w_in": bell_draw(key_list[2], (IN_WIDTH, HIDDEN_SIZE), IN_WIDTH ** -0.5, 0.25),
        "b_in": bell_draw(key_list[3], (HIDDEN_SIZE,), 0.5, 3.0, (), jnp.float32),
        "w_out": bell_draw(key_list[4], (LEVELS, HIDDEN_SIZE), HIDDEN_SIZE ** -0.5, 0.1875),
        "edge_flips": set_ends((jax.random.randint(key_list[5], (TILES, 2), 0, 2) < 1).astype(jnp.int32), jax.random.fold_in(key_list[5], 1), 0, 1),
    }


STEP_SIZE = 0.25


def pad_tiles(current, edge_flips):
    west_col = jnp.roll(current[..., SIDE - 1:], 1, axis=0)
    east_col = jnp.roll(current[..., :1], -1, axis=0)
    extended = jnp.concatenate([west_col, current, east_col], axis=3)
    north_row = jnp.roll(extended[:, :, SIDE - 1, :], TILE_ROW, axis=0)
    south_row = jnp.roll(extended[:, :, 0, :], -TILE_ROW, axis=0)
    north_row = jnp.where(edge_flips[:, 0][:, None, None] == 1, north_row[..., ::-1], north_row)
    south_row = jnp.where(edge_flips[:, 1][:, None, None] == 1, south_row[..., ::-1], south_row)
    return jnp.concatenate([north_row[:, :, None], extended, south_row[:, :, None]], axis=2)


def unpad_tiles(pad_grad, edge_flips):
    extended = pad_grad[:, :, 1:-1, :]
    north_grad = pad_grad[:, :, 0, :]
    south_grad = pad_grad[:, :, -1, :]
    north_grad = jnp.where(edge_flips[:, 0][:, None, None] == 1, north_grad[..., ::-1], north_grad)
    south_grad = jnp.where(edge_flips[:, 1][:, None, None] == 1, south_grad[..., ::-1], south_grad)
    extended = extended.at[:, :, SIDE - 1, :].add(jnp.roll(north_grad, -TILE_ROW, axis=0))
    extended = extended.at[:, :, 0, :].add(jnp.roll(south_grad, TILE_ROW, axis=0))
    inner = extended[..., 1:-1]
    inner = inner.at[..., SIDE - 1].add(jnp.roll(extended[..., 0], -1, axis=0))
    inner = inner.at[..., 0].add(jnp.roll(extended[..., -1], 1, axis=0))
    return inner


def gather_patches(padded):
    pieces = [padded[:, :, row_shift:row_shift + SIDE, col_shift:col_shift + SIDE]
              for row_shift in range(3) for col_shift in range(3)]
    return jnp.stack(pieces, axis=1).reshape(TILES, 9 * LEVELS, COLS)


def scatter_patches(patch_grad):
    pieces = patch_grad.reshape(TILES, 9, LEVELS, SIDE, SIDE)
    total = jnp.zeros((TILES, LEVELS, SIDE + 2, SIDE + 2), jnp.float32)
    for row_shift in range(3):
        for col_shift in range(3):
            total = total + jnp.pad(pieces[:, 3 * row_shift + col_shift],
                                    ((0, 0), (0, 0), (row_shift, 2 - row_shift), (col_shift, 2 - col_shift)))
    return total


def reference(initial_state, cotangent, w_in, b_in, w_out, edge_flips):
    w_in32 = w_in.astype(jnp.float32)
    w_out32 = w_out.astype(jnp.float32)
    current = initial_state.reshape(TILES, LEVELS, SIDE, SIDE)
    saved_fields = []
    for step_index in range(STEPS):
        saved_fields.append(current)
        patch_vals = gather_patches(pad_tiles(current, edge_flips)).astype(jnp.bfloat16)
        pre_act = jnp.einsum('ih,nic->nhc', w_in32, patch_vals.astype(jnp.float32)) + b_in[None, :, None]
        hidden_vals = jax.nn.silu(pre_act).astype(jnp.bfloat16)
        tendency = jnp.einsum('lh,nhc->nlc', w_out32, hidden_vals.astype(jnp.float32))
        level_mean = jnp.sum(tendency, axis=(0, 2)) / (TILES * COLS)
        current = current + (STEP_SIZE * (tendency - level_mean[None, :, None])).reshape(current.shape)
    final_state = current.reshape(TILES, LEVELS, COLS)
    gradient = cotangent
    grad_w_in = jnp.zeros((IN_WIDTH, HIDDEN_SIZE), jnp.float32)
    grad_w_out = jnp.zeros((LEVELS, HIDDEN_SIZE), jnp.float32)
    grad_b_in = jnp.zeros((HIDDEN_SIZE,), jnp.float32)
    for step_index in reversed(range(STEPS)):
        patch_vals = gather_patches(pad_tiles(saved_fields[step_index], edge_flips)).astype(jnp.bfloat16)
        pre_act = jnp.einsum('ih,nic->nhc', w_in32, patch_vals.astype(jnp.float32)) + b_in[None, :, None]
        hidden_vals = jax.nn.silu(pre_act).astype(jnp.bfloat16)
        scaled = STEP_SIZE * gradient
        level_grad = jnp.sum(scaled, axis=(0, 2)) / (TILES * COLS)
        tend_grad = (scaled - level_grad[None, :, None]).astype(jnp.bfloat16).astype(jnp.float32)
        grad_w_out = grad_w_out + jnp.einsum('nlc,nhc->lh', tend_grad, hidden_vals.astype(jnp.float32))
        hidden_grad = jnp.einsum('lh,nlc->nhc', w_out32, tend_grad)
        sigmoid_vals = jax.nn.sigmoid(pre_act)
        pre_grad = hidden_grad * sigmoid_vals * (1.0 + pre_act * (1.0 - sigmoid_vals))
        grad_b_in = grad_b_in + jnp.sum(pre_grad, axis=(0, 2))
        pre_low = pre_grad.astype(jnp.bfloat16).astype(jnp.float32)
        grad_w_in = grad_w_in + jnp.einsum('nic,nhc->ih', patch_vals.astype(jnp.float32), pre_low)
        patch_grad = jnp.einsum('ih,nhc->nic', w_in32, pre_low)
        gradient = gradient + unpad_tiles(scatter_patches(patch_grad), edge_flips).reshape(TILES, LEVELS, COLS)
    return (final_state, gradient, grad_w_in, grad_b_in, grad_w_out)
```

```python
import functools

import jax
import jax.numpy as jnp
from jax import lax
from jax.experimental import pallas as pl
from jax.experimental.pallas import tpu as pltpu
from jax.sharding import PartitionSpec as P

STEPS = 4
TILE_ROW = 4
STEP_SIZE = 0.25
LEAD = 8
MESH = pl.DeviceIdType.MESH
F32 = jnp.float32
BF16 = jnp.bfloat16

PIECES = {}
TOTAL_ROWS = 0


def layout(width, rows):
    names = [("N", width), ("S", width), ("W", rows), ("E", rows)]
    names += [(name, 8) for name in ("NW", "NE", "SW", "SE")]
    place, at = {}, 0
    for name, size in names:
        place[name] = (at, size)
        at += size
    return place, at


def dot(a, b, dims, precision=None):
    return lax.dot_general(a, b, (dims, ((), ())), preferred_element_type=F32, precision=precision)


def chain_kernel(
    tiles, subs, rows, width, levels, hidden,
    state_ref, cot_ref, w_in_ref, b_in_ref, w_out_ref, flips_ref,
    final_ref, grad_ref, gw_in_ref, gb_ref, gw_out_ref,
    send, recv, tile_out, tile_in, sub_out, sub_in,
    padded, pad_grad, edge, field, gradient, totals, pre, hid, slope, patch,
    gp16, gt16,
    halo_ssem, halo_rsem, tile_ssem, tile_rsem, sub_ssem, sub_rsem,
):
    place, _ = layout(width, rows)
    cols = rows * width
    inv_total = 1.0 / (tiles * subs * cols)
    me_t, me_s = lax.axis_index("tile"), lax.axis_index("sub")
    first, last = me_s == 0, me_s == subs - 1
    wide = width + 2 * LEAD

    def tile_at(by):
        return lax.rem(me_t + by + 2 * tiles, tiles)

    def north_of(by):
        return (jnp.where(first, tile_at(by - TILE_ROW), tile_at(by)), jnp.where(first, subs - 1, me_s - 1))

    def south_of(by):
        return (jnp.where(last, tile_at(by + TILE_ROW), tile_at(by)), jnp.where(last, 0, me_s + 1))

    targets = {
        "N": north_of(0), "S": south_of(0), "W": (tile_at(-1), me_s), "E": (tile_at(1), me_s),
        "NW": north_of(-1), "NE": north_of(1), "SW": south_of(-1), "SE": south_of(1),
    }

    def halo_copies(p):
        out = []
        for i, (name, (at, size)) in enumerate(place.items()):
            out.append(pltpu.make_async_remote_copy(
                src_ref=send.at[p, pl.ds(at, size)], dst_ref=recv.at[p, pl.ds(at, size)],
                send_sem=halo_ssem.at[p, i], recv_sem=halo_rsem.at[p, i],
                device_id=targets[name], device_id_type=MESH))
        return out

    def tile_copies(p):
        return [pltpu.make_async_remote_copy(
            src_ref=tile_out.at[p], dst_ref=tile_in.at[p, d - 1],
            send_sem=tile_ssem.at[p, d - 1], recv_sem=tile_rsem.at[p, d - 1],
            device_id=(tile_at(d), me_s), device_id_type=MESH) for d in range(1, tiles)]

    def sub_copies(p):
        return [pltpu.make_async_remote_copy(
            src_ref=sub_out.at[p], dst_ref=sub_in.at[p, d - 1],
            send_sem=sub_ssem.at[p, d - 1], recv_sem=sub_rsem.at[p, d - 1],
            device_id=(me_t, lax.rem(me_s + d, subs)), device_id_type=MESH) for d in range(1, subs)]

    def start_exchange(p):
        for copy in tile_copies(p) + halo_copies(p):
            copy.start()

    def finish_exchange(p):
        for copy in tile_copies(p):
            copy.wait()
        total = tile_out[p]
        for d in range(1, tiles):
            total = total + tile_in[p, d - 1]
        sub_out[p] = total
        for copy in sub_copies(p):
            copy.start()
        for copy in halo_copies(p):
            copy.wait()
        for copy in sub_copies(p):
            copy.wait()
        for d in range(1, subs):
            total = total + sub_in[p, d - 1]
        return total

    at_row = lax.broadcasted_iota(jnp.int32, (wide, wide), 0)
    at_col = lax.broadcasted_iota(jnp.int32, (wide, wide), 1)
    same = (at_row == at_col).astype(F32)
    turned = (at_row + at_col == wide - 1).astype(F32)

    def seam_matrix(flag, here):
        mix = jnp.where(here, flag, 0).astype(F32)
        return turned * mix + same * (1.0 - mix)

    turn_north = seam_matrix(flips_ref[0, 0], first)
    turn_south = seam_matrix(flips_ref[0, 1], last)

    def send_field(p):
        for name, row in (("N", 0), ("S", rows - 1)):
            at = place[name][0]
            line = field[row * width:(row + 1) * width]
            send[p, at:at + width] = line
            for side, cell in (("W", 0), ("E", width - 1)):
                corner = place[name + side][0]
                send[p, corner:corner + 1] = line[cell:cell + 1]
        for name, cell in (("W", 0), ("E", width - 1)):
            at = place[name][0]
            for r in range(rows):
                send[p, at + r:at + r + 1] = field[r * width + cell:r * width + cell + 1]

    def pad_field(p, shift):
        padded[1:rows + 1, LEAD:LEAD + width, :] = (field[...]).reshape(rows, width, levels)
        for name, cell in (("E", LEAD - 1), ("W", LEAD + width)):
            at = place[name][0]
            for r in range(rows):
                padded[r + 1, cell:cell + 1] = recv[p, at + r:at + r + 1] - shift
        for name, row, turn in (("S", 0, turn_north), ("N", rows + 1, turn_south)):
            at = place[name][0]
            edge[LEAD:LEAD + width] = recv[p, at:at + width] - shift
            for side, cell in (("E", LEAD - 1), ("W", LEAD + width)):
                corner = place[name + side][0]
                edge[cell:cell + 1] = recv[p, corner:corner + 1] - shift
            padded[row] = dot(turn.astype(BF16), edge[...].astype(BF16), ((1,), (0,)))

    send[...] = jnp.zeros_like(send)
    tile_out[...] = jnp.zeros_like(tile_out)
    edge[...] = jnp.zeros_like(edge)
    field[...] = state_ref[0].T
    gradient[...] = cot_ref[0].T
    send_field(0)
    tile_out[0, 1:2] = jnp.sum(gradient[...], axis=0, keepdims=True)
    start_exchange(0)
    gw_in_ref[...] = jnp.zeros_like(gw_in_ref)
    gb_ref[...] = jnp.zeros_like(gb_ref)
    gw_out_ref[...] = jnp.zeros_like(gw_out_ref)
    padded[...] = jnp.zeros_like(padded)

    def forward(k, carry):
        total = finish_exchange(k)
        shift = total[0:1] * (STEP_SIZE * inv_total)
        field[...] = field[...] - shift

        @pl.when(k == 0)
        def _():
            totals[...] = total

        pad_field(k, shift)
        for a in range(3):
            for b in range(3):
                o = 3 * a + b
                piece = padded[a:a + rows, LEAD - 1 + b:LEAD - 1 + b + width, :]
                patch[k, :, o * levels:(o + 1) * levels] = piece.reshape(cols, levels).astype(BF16)
        act = dot(patch[k], w_in_ref[...], ((1,), (0,))) + b_in_ref[...]
        pre[...] = act
        low = (act * jax.nn.sigmoid(act)).astype(BF16)
        hid[k] = low
        tendency = dot(low, w_out_ref[...], ((1,), (1,)))
        field[...] = field[...] + STEP_SIZE * tendency
        tile_out[k + 1, 0:1] = jnp.sum(tendency, axis=0, keepdims=True)

        @pl.when(k < STEPS - 1)
        def _():
            send_field(k + 1)
            start_exchange(k + 1)

        value = pre[...]
        sig = jax.nn.sigmoid(value)
        slope[k] = sig * (1.0 + value * (1.0 - sig))
        return carry

    lax.fori_loop(0, STEPS, forward, 0)

    def backward(j, carry):
        k = STEPS - 1 - j
        p = STEPS + j
        level_grad = totals[1:2] * (STEP_SIZE * inv_total)
        low_gt = (STEP_SIZE * gradient[...] - level_grad).astype(BF16)
        gt16[...] = low_gt
        gh = dot(low_gt, w_out_ref[...], ((1,), (0,)))
        gp = gh * slope[k]
        pre[...] = gp
        low = gp.astype(BF16)
        gp16[...] = low
        gi = dot(low, w_in_ref[...], ((1,), (1,)))
        pad_grad[...] = jnp.zeros_like(pad_grad)
        for a in range(3):
            for b in range(3):
                o = 3 * a + b
                piece = gi[:, o * levels:(o + 1) * levels].reshape(rows, width, levels)
                pad_grad[a:a + rows, LEAD - 1 + b:LEAD - 1 + b + width, :] += piece
        whole = jnp.sum(gi, axis=0, keepdims=True)
        part = whole[:, 0:levels]
        for o in range(1, 9):
            part = part + whole[:, o * levels:(o + 1) * levels]
        tile_out[p, 1:2] = part
        for name, row, turn in (("N", 0, turn_north), ("S", rows + 1, turn_south)):
            at = place[name][0]
            edge[...] = dot(turn, pad_grad[row], ((1,), (0,)), lax.Precision.HIGHEST)
            send[p, at:at + width] = edge[LEAD:LEAD + width]
            for side, cell in (("W", LEAD - 1), ("E", LEAD + width)):
                corner = place[name + side][0]
                send[p, corner:corner + 1] = edge[cell:cell + 1]
        for name, cell in (("W", LEAD - 1), ("E", LEAD + width)):
            at = place[name][0]
            for r in range(rows):
                send[p, at + r:at + r + 1] = pad_grad[r + 1, cell:cell + 1]
        start_exchange(p)
        gradient[...] += pad_grad[1:rows + 1, LEAD:LEAD + width, :].reshape(cols, levels)
        gw_in_ref[...] += dot(patch[k], gp16[...], ((0,), (0,)))
        gw_out_ref[...] += dot(gt16[...], hid[k], ((0,), (0,)))
        gb_ref[...] += jnp.sum(pre[...], axis=0, keepdims=True)
        total = finish_exchange(p)

        @pl.when(j == 0)
        def _():
            field[...] = field[...] - total[0:1] * (STEP_SIZE * inv_total)

        totals[1:2] = totals[1:2] + total[1:2]
        for name, row in (("N", rows - 1), ("S", 0)):
            at = place[name][0]
            gradient[row * width:(row + 1) * width] += recv[p, at:at + width]
            for side, cell in (("W", width - 1), ("E", 0)):
                corner = place[name + side][0]
                gradient[row * width + cell:row * width + cell + 1] += recv[p, corner:corner + 1]
        for name, cell in (("W", width - 1), ("E", 0)):
            at = place[name][0]
            for r in range(rows):
                gradient[r * width + cell:r * width + cell + 1] += recv[p, at + r:at + r + 1]
        return carry

    lax.fori_loop(0, STEPS, backward, 0)
    final_ref[0] = field[...].T
    grad_ref[0] = gradient[...].T


def shards(tiles, subs, initial_state, cotangent, w_in, b_in, w_out, edge_flips):
    _, levels, cols = initial_state.shape
    in_width, hidden = w_in.shape
    side = 1
    while side * side < cols * subs:
        side += 1
    rows, width = side // subs, side
    _, buffer_rows = layout(width, rows)
    phases = 2 * STEPS
    wide = width + 2 * LEAD
    vmem = pl.BlockSpec(memory_space=pltpu.VMEM)
    final, grad, gw_in, gb, gw_out = pl.pallas_call(
        functools.partial(chain_kernel, tiles, subs, rows, width, levels, hidden),
        out_shape=(
            jax.ShapeDtypeStruct(initial_state.shape, F32),
            jax.ShapeDtypeStruct(initial_state.shape, F32),
            jax.ShapeDtypeStruct((in_width, hidden), F32),
            jax.ShapeDtypeStruct((1, hidden), F32),
            jax.ShapeDtypeStruct((levels, hidden), F32),
        ),
        in_specs=[vmem] * 5 + [pl.BlockSpec(memory_space=pltpu.SMEM)],
        out_specs=[vmem] * 5,
        scratch_shapes=[
            pltpu.VMEM((phases, buffer_rows, levels), F32),
            pltpu.VMEM((phases, buffer_rows, levels), F32),
            pltpu.VMEM((phases, 8, levels), F32),
            pltpu.VMEM((phases, tiles - 1, 8, levels), F32),
            pltpu.VMEM((phases, 8, levels), F32),
            pltpu.VMEM((phases, subs - 1, 8, levels), F32),
            pltpu.VMEM((rows + 2, wide, levels), F32),
            pltpu.VMEM((rows + 2, wide, levels), F32),
            pltpu.VMEM((wide, levels), F32),
            pltpu.VMEM((cols, levels), F32),
            pltpu.VMEM((cols, levels), F32),
            pltpu.VMEM((8, levels), F32),
            pltpu.VMEM((cols, hidden), F32),
            pltpu.VMEM((STEPS, cols, hidden), BF16),
            pltpu.VMEM((STEPS, cols, hidden), F32),
            pltpu.VMEM((STEPS, cols, in_width), BF16),
            pltpu.VMEM((cols, hidden), BF16),
            pltpu.VMEM((cols, levels), BF16),
            pltpu.SemaphoreType.DMA((phases, 8)),
            pltpu.SemaphoreType.DMA((phases, 8)),
            pltpu.SemaphoreType.DMA((phases, tiles - 1)),
            pltpu.SemaphoreType.DMA((phases, tiles - 1)),
            pltpu.SemaphoreType.DMA((phases, subs - 1)),
            pltpu.SemaphoreType.DMA((phases, subs - 1)),
        ],
        compiler_params=pltpu.CompilerParams(has_side_effects=True, vmem_limit_bytes=48 * 1024 * 1024),
        name="chain",
    )(initial_state, cotangent, w_in, b_in[None, :], w_out, edge_flips)
    stacked = jnp.concatenate([gw_in, gw_out, gb, jnp.zeros((7, hidden), F32)], axis=0)
    part = lax.psum_scatter(stacked, "sub", scatter_dimension=1, tiled=True)
    part = lax.psum(part, "tile")
    full = lax.all_gather(part.astype(BF16), "sub", axis=1, tiled=True).astype(F32)
    return (final, grad, full[:in_width], full[in_width + levels], full[in_width:in_width + levels])


def solution(mesh):
    in_specs = (P("tile", None, "sub"), P("tile", None, "sub"), P(), P(), P(), P("tile", None))
    out_specs = (P("tile", None, "sub"), P("tile", None, "sub"), P(), P(), P())
    body = functools.partial(shards, mesh.shape["tile"], mesh.shape["sub"])
    return jax.shard_map(body, mesh=mesh, in_specs=in_specs, out_specs=out_specs, check_vma=False)
```

```python
import functools

import jax
import jax.numpy as jnp
from jax import lax
from jax.experimental import pallas as pl
from jax.experimental.pallas import tpu as pltpu
from jax.sharding import PartitionSpec as P

STEPS = 4
TILE_ROW = 4
STEP_SIZE = 0.25
LEAD = 8
MESH = pl.DeviceIdType.MESH
F32 = jnp.float32
BF16 = jnp.bfloat16

LANES = 128
DIRECT_LIMIT = 64


def layout(width, rows):
    names = [("N", width), ("S", width), ("W", rows), ("E", rows)]
    names += [(name, 8) for name in ("NW", "NE", "SW", "SE")]
    place, at = {}, 0
    for name, size in names:
        place[name] = (at, size)
        at += size
    return place, at


def reduce_plan(tiles, subs, flat_rows):
    bits = [("sub", 1 << i) for i in range(subs.bit_length() - 1)]
    bits += [("tile", 1 << i) for i in range(tiles.bit_length() - 1)]
    unit = 16 * tiles * subs
    units = -(-flat_rows // unit)
    count = min(3, units)
    groups, at = [], 0
    for g in range(count):
        size = (units // count + (1 if g < units % count else 0)) * unit
        turning = bits[1:4]
        order = bits[:1] + turning[g:] + turning[:g] + bits[4:]
        groups.append((at, size, order))
        at += size
    return groups, at


def dot(a, b, dims, precision=None):
    return lax.dot_general(a, b, (dims, ((), ())), preferred_element_type=F32, precision=precision)


def chain_kernel(
    tiles, subs, rows, width, levels, hidden,
    state_ref, cot_ref, w_in_ref, b_in_ref, w_out_ref, flips_ref,
    final_ref, grad_ref, gw_in_ref, gb_ref, gw_out_ref,
    flat, out_half, in_half, whole, red_ssem, red_rsem, gat_ssem, gat_rsem,
    bias_out, bias_tiles, bias_subs, bias_ssem, bias_rsem, side_ssem, side_rsem,
    send, recv, tile_out, tile_in, sub_out, sub_in,
    padded, pad_grad, edge, field, gradient, totals, pre, hid, slope, patch,
    gp16, gt16,
    halo_ssem, halo_rsem, tile_ssem, tile_rsem, sub_ssem, sub_rsem,
):
    place, _ = layout(width, rows)
    cols = rows * width
    inv_total = 1.0 / (tiles * subs * cols)
    me_t, me_s = lax.axis_index("tile"), lax.axis_index("sub")
    first, last = me_s == 0, me_s == subs - 1
    wide = width + 2 * LEAD

    def tile_at(by):
        return lax.rem(me_t + by + 2 * tiles, tiles)

    def north_of(by):
        return (jnp.where(first, tile_at(by - TILE_ROW), tile_at(by)), jnp.where(first, subs - 1, me_s - 1))

    def south_of(by):
        return (jnp.where(last, tile_at(by + TILE_ROW), tile_at(by)), jnp.where(last, 0, me_s + 1))

    targets = {
        "N": north_of(0), "S": south_of(0), "W": (tile_at(-1), me_s), "E": (tile_at(1), me_s),
        "NW": north_of(-1), "NE": north_of(1), "SW": south_of(-1), "SE": south_of(1),
    }

    def halo_copies(p):
        out = []
        for i, (name, (at, size)) in enumerate(place.items()):
            out.append(pltpu.make_async_remote_copy(
                src_ref=send.at[p, pl.ds(at, size)], dst_ref=recv.at[p, pl.ds(at, size)],
                send_sem=halo_ssem.at[p, i], recv_sem=halo_rsem.at[p, i],
                device_id=targets[name], device_id_type=MESH))
        return out

    direct = tiles * subs <= DIRECT_LIMIT
    me = me_t * subs + me_s

    def sum_copies(p):
        out = []
        for d in range(1, tiles * subs if direct else tiles):
            if direct:
                peer = lax.rem(me + d, tiles * subs)
                there = (peer // subs, lax.rem(peer, subs))
            else:
                there = (tile_at(d), me_s)
            out.append(pltpu.make_async_remote_copy(
                src_ref=tile_out.at[p], dst_ref=tile_in.at[p, d - 1],
                send_sem=tile_ssem.at[p, d - 1], recv_sem=tile_rsem.at[p, d - 1],
                device_id=there, device_id_type=MESH))
        return out

    def sub_copies(p):
        return [pltpu.make_async_remote_copy(
            src_ref=sub_out.at[p], dst_ref=sub_in.at[p, d - 1],
            send_sem=sub_ssem.at[p, d - 1], recv_sem=sub_rsem.at[p, d - 1],
            device_id=(me_t, lax.rem(me_s + d, subs)), device_id_type=MESH) for d in range(1, subs)]

    def start_exchange(p):
        for copy in sum_copies(p) + halo_copies(p):
            copy.start()

    def finish_exchange(p):
        for copy in sum_copies(p):
            copy.wait()
        total = tile_out[p]
        for d in range(1, tiles * subs if direct else tiles):
            total = total + tile_in[p, d - 1]
        if not direct:
            sub_out[p] = total
            for copy in sub_copies(p):
                copy.start()
        for copy in halo_copies(p):
            copy.wait()
        if not direct:
            for copy in sub_copies(p):
                copy.wait()
            for d in range(1, subs):
                total = total + sub_in[p, d - 1]
        return total

    at_row = lax.broadcasted_iota(jnp.int32, (wide, wide), 0)
    at_col = lax.broadcasted_iota(jnp.int32, (wide, wide), 1)
    same = (at_row == at_col).astype(F32)
    turned = (at_row + at_col == wide - 1).astype(F32)

    def seam_matrix(flag, here):
        mix = jnp.where(here, flag, 0).astype(F32)
        return turned * mix + same * (1.0 - mix)

    turn_north = seam_matrix(flips_ref[0, 0], first)
    turn_south = seam_matrix(flips_ref[0, 1], last)

    def send_field(p):
        for name, row in (("N", 0), ("S", rows - 1)):
            at = place[name][0]
            line = field[row * width:(row + 1) * width]
            send[p, at:at + width] = line
            for side, cell in (("W", 0), ("E", width - 1)):
                corner = place[name + side][0]
                send[p, corner:corner + 1] = line[cell:cell + 1]
        for name, cell in (("W", 0), ("E", width - 1)):
            at = place[name][0]
            for r in range(rows):
                send[p, at + r:at + r + 1] = field[r * width + cell:r * width + cell + 1]

    def pad_field(p, shift):
        padded[1:rows + 1, LEAD:LEAD + width, :] = (field[...]).reshape(rows, width, levels)
        for name, cell in (("E", LEAD - 1), ("W", LEAD + width)):
            at = place[name][0]
            for r in range(rows):
                padded[r + 1, cell:cell + 1] = recv[p, at + r:at + r + 1] - shift
        for name, row, turn in (("S", 0, turn_north), ("N", rows + 1, turn_south)):
            at = place[name][0]
            edge[LEAD:LEAD + width] = recv[p, at:at + width] - shift
            for side, cell in (("E", LEAD - 1), ("W", LEAD + width)):
                corner = place[name + side][0]
                edge[cell:cell + 1] = recv[p, corner:corner + 1] - shift
            padded[row] = dot(turn.astype(BF16), edge[...].astype(BF16), ((1,), (0,)))

    send[...] = jnp.zeros_like(send)
    tile_out[...] = jnp.zeros_like(tile_out)
    edge[...] = jnp.zeros_like(edge)
    field[...] = state_ref[0].T
    gradient[...] = cot_ref[0].T
    send_field(0)
    tile_out[0, 1:2] = jnp.sum(gradient[...], axis=0, keepdims=True)
    start_exchange(0)
    gw_in_ref[...] = jnp.zeros_like(gw_in_ref)
    gb_ref[...] = jnp.zeros_like(gb_ref)
    gw_out_ref[...] = jnp.zeros_like(gw_out_ref)
    padded[...] = jnp.zeros_like(padded)

    def forward(k, carry):
        total = finish_exchange(k)
        shift = total[0:1] * (STEP_SIZE * inv_total)
        field[...] = field[...] - shift

        @pl.when(k == 0)
        def _():
            totals[...] = total

        pad_field(k, shift)
        for a in range(3):
            for b in range(3):
                o = 3 * a + b
                piece = padded[a:a + rows, LEAD - 1 + b:LEAD - 1 + b + width, :]
                patch[k, :, o * levels:(o + 1) * levels] = piece.reshape(cols, levels).astype(BF16)
        act = dot(patch[k], w_in_ref[...], ((1,), (0,))) + b_in_ref[...]
        pre[...] = act
        low = (act * jax.nn.sigmoid(act)).astype(BF16)
        hid[k] = low
        tendency = dot(low, w_out_ref[...], ((1,), (1,)))
        field[...] = field[...] + STEP_SIZE * tendency
        tile_out[k + 1, 0:1] = jnp.sum(tendency, axis=0, keepdims=True)

        @pl.when(k < STEPS - 1)
        def _():
            send_field(k + 1)
            start_exchange(k + 1)

        value = pre[...]
        sig = jax.nn.sigmoid(value)
        slope[k] = sig * (1.0 + value * (1.0 - sig))
        return carry

    lax.fori_loop(0, STEPS, forward, 0)

    def backward(j, carry):
        k = STEPS - 1 - j
        p = STEPS + j
        level_grad = totals[1:2] * (STEP_SIZE * inv_total)
        low_gt = (STEP_SIZE * gradient[...] - level_grad).astype(BF16)
        gt16[...] = low_gt
        gh = dot(low_gt, w_out_ref[...], ((1,), (0,)))
        gp = gh * slope[k]
        pre[...] = gp
        low = gp.astype(BF16)
        gp16[...] = low
        gi = dot(low, w_in_ref[...], ((1,), (1,)))
        pad_grad[...] = jnp.zeros_like(pad_grad)
        for a in range(3):
            for b in range(3):
                o = 3 * a + b
                piece = gi[:, o * levels:(o + 1) * levels].reshape(rows, width, levels)
                pad_grad[a:a + rows, LEAD - 1 + b:LEAD - 1 + b + width, :] += piece
        gi_sum = jnp.sum(gi, axis=0, keepdims=True)
        part = gi_sum[:, 0:levels]
        for o in range(1, 9):
            part = part + gi_sum[:, o * levels:(o + 1) * levels]
        tile_out[p, 1:2] = part
        for name, row, turn in (("N", 0, turn_north), ("S", rows + 1, turn_south)):
            at = place[name][0]
            edge[...] = dot(turn, pad_grad[row], ((1,), (0,)), lax.Precision.HIGHEST)
            send[p, at:at + width] = edge[LEAD:LEAD + width]
            for side, cell in (("W", LEAD - 1), ("E", LEAD + width)):
                corner = place[name + side][0]
                send[p, corner:corner + 1] = edge[cell:cell + 1]
        for name, cell in (("W", LEAD - 1), ("E", LEAD + width)):
            at = place[name][0]
            for r in range(rows):
                send[p, at + r:at + r + 1] = pad_grad[r + 1, cell:cell + 1]
        start_exchange(p)
        gradient[...] += pad_grad[1:rows + 1, LEAD:LEAD + width, :].reshape(cols, levels)
        gw_in_ref[...] += dot(patch[k], gp16[...], ((0,), (0,)))
        gw_out_ref[...] += dot(gt16[...], hid[k], ((0,), (0,)))
        gb_ref[...] += jnp.sum(pre[...], axis=0, keepdims=True)
        total = finish_exchange(p)

        @pl.when(j == 0)
        def _():
            field[...] = field[...] - total[0:1] * (STEP_SIZE * inv_total)

        totals[1:2] = totals[1:2] + total[1:2]
        for name, row in (("N", rows - 1), ("S", 0)):
            at = place[name][0]
            gradient[row * width:(row + 1) * width] += recv[p, at:at + width]
            for side, cell in (("W", width - 1), ("E", 0)):
                corner = place[name + side][0]
                gradient[row * width + cell:row * width + cell + 1] += recv[p, corner:corner + 1]
        for name, cell in (("W", width - 1), ("E", 0)):
            at = place[name][0]
            for r in range(rows):
                gradient[r * width + cell:r * width + cell + 1] += recv[p, at + r:at + r + 1]
        return carry

    lax.fori_loop(0, STEPS, backward, 0)

    in_width = gw_in_ref.shape[0]
    stride = in_width + levels
    for c in range(hidden // LANES):
        bias_out[0, c:c + 1] = gb_ref[:, c * LANES:(c + 1) * LANES]
    bias_tiles[me_t] = bias_out[0]

    def bias_tile_copies():
        return [pltpu.make_async_remote_copy(
            src_ref=bias_out.at[0], dst_ref=bias_tiles.at[me_t],
            send_sem=bias_ssem.at[d - 1], recv_sem=bias_rsem.at[d - 1],
            device_id=(tile_at(d), me_s), device_id_type=MESH) for d in range(1, tiles)]

    def bias_sub_copies():
        return [pltpu.make_async_remote_copy(
            src_ref=bias_out.at[1], dst_ref=bias_subs.at[me_s],
            send_sem=side_ssem.at[d - 1], recv_sem=side_rsem.at[d - 1],
            device_id=(me_t, lax.rem(me_s + d, subs)), device_id_type=MESH) for d in range(1, subs)]

    for copy in bias_tile_copies():
        copy.start()
    groups, flat_rows = reduce_plan(tiles, subs, stride * (hidden // LANES))
    for c in range(hidden // LANES):
        at, lanes = c * stride, slice(c * LANES, (c + 1) * LANES)
        flat[at:at + in_width] = gw_in_ref[:, lanes]
        flat[at + in_width:at + in_width + levels] = gw_out_ref[:, lanes]
    used = stride * (hidden // LANES)
    if flat_rows > used:
        flat[used:flat_rows] = jnp.zeros((flat_rows - used, LANES), F32)

    def bit_of(axis, step):
        index = me_t if axis == "tile" else me_s
        return lax.rem(index // step, 2)

    def peer_of(axis, step):
        if axis == "tile":
            return (me_t + step * (1 - 2 * bit_of(axis, step)), me_s)
        return (me_t, me_s + step * (1 - 2 * bit_of(axis, step)))

    def bases(group):
        start, size, order = group
        out, base = [], start
        for axis, step in order:
            out.append((base, size // 2))
            size = size // 2
            base = base + bit_of(axis, step) * size
        return out, base, size

    depth = len(groups[0][2])

    def reduce_copy(g, i):
        start, size, order = groups[g]
        half = size >> (i + 1)
        at = start + size - (size >> i)
        return pltpu.make_async_remote_copy(
            src_ref=out_half.at[pl.ds(at, half)], dst_ref=in_half.at[pl.ds(at, half)],
            send_sem=red_ssem.at[g, i], recv_sem=red_rsem.at[g, i],
            device_id=peer_of(*order[i]), device_id_type=MESH)

    def gather_copy(g, i):
        start, size, order = groups[g]
        part = size >> (i + 1)
        base = bases(groups[g])[0][i][0] + bit_of(*order[i]) * part
        rows_here = pl.ds(pl.multiple_of(base, 16), part)
        return pltpu.make_async_remote_copy(
            src_ref=whole.at[rows_here], dst_ref=whole.at[rows_here],
            send_sem=gat_ssem.at[g, i], recv_sem=gat_rsem.at[g, i],
            device_id=peer_of(*order[i]), device_id_type=MESH)

    for i in range(depth + 1):
        for g, (start, size, order) in enumerate(groups):
            levels_of = bases((start, size, order))
            if i > 0:
                reduce_copy(g, i - 1).wait()
                base, half = levels_of[0][i - 1]
                at = start + size - (size >> (i - 1))
                kept = pl.ds(pl.multiple_of(base + bit_of(*order[i - 1]) * half, 16), half)
                flat[kept] = flat[kept] + in_half[at:at + half].astype(F32)
            if i < depth:
                base, half = levels_of[0][i]
                at = start + size - (size >> i)
                away = pl.ds(pl.multiple_of(base + (1 - bit_of(*order[i])) * half, 16), half)
                out_half[at:at + half] = flat[away].astype(BF16)
                reduce_copy(g, i).start()
            else:
                own = pl.ds(pl.multiple_of(levels_of[1], 16), levels_of[2])
                whole[own] = flat[own].astype(BF16)
                gather_copy(g, depth - 1).start()
    for copy in bias_tile_copies():
        copy.wait()
    bias = bias_tiles[0]
    for d in range(1, tiles):
        bias = bias + bias_tiles[d]
    bias_out[1] = bias
    bias_subs[me_s] = bias
    for copy in bias_sub_copies():
        copy.start()
    for i in reversed(range(depth)):
        for g in range(len(groups)):
            gather_copy(g, i).wait()
            if i > 0:
                gather_copy(g, i - 1).start()
    for copy in bias_sub_copies():
        copy.wait()
    bias = bias_subs[0]
    for d in range(1, subs):
        bias = bias + bias_subs[d]
    for c in range(hidden // LANES):
        at, lanes = c * stride, slice(c * LANES, (c + 1) * LANES)
        gw_in_ref[:, lanes] = whole[at:at + in_width].astype(F32)
        gw_out_ref[:, lanes] = whole[at + in_width:at + in_width + levels].astype(F32)
        gb_ref[:, lanes] = bias[c:c + 1]
    final_ref[0] = field[...].T
    grad_ref[0] = gradient[...].T


def shards(tiles, subs, initial_state, cotangent, w_in, b_in, w_out, edge_flips):
    _, levels, cols = initial_state.shape
    in_width, hidden = w_in.shape
    side = 1
    while side * side < cols * subs:
        side += 1
    rows, width = side // subs, side
    _, buffer_rows = layout(width, rows)
    phases = 2 * STEPS
    groups, flat_rows = reduce_plan(tiles, subs, (in_width + levels) * (hidden // LANES))
    depth = len(groups[0][2])
    fan = tiles * subs - 1 if tiles * subs <= DIRECT_LIMIT else tiles - 1
    wide = width + 2 * LEAD
    vmem = pl.BlockSpec(memory_space=pltpu.VMEM)
    final, grad, gw_in, gb, gw_out = pl.pallas_call(
        functools.partial(chain_kernel, tiles, subs, rows, width, levels, hidden),
        out_shape=(
            jax.ShapeDtypeStruct(initial_state.shape, F32),
            jax.ShapeDtypeStruct(initial_state.shape, F32),
            jax.ShapeDtypeStruct((in_width, hidden), F32),
            jax.ShapeDtypeStruct((1, hidden), F32),
            jax.ShapeDtypeStruct((levels, hidden), F32),
        ),
        in_specs=[vmem] * 5 + [pl.BlockSpec(memory_space=pltpu.SMEM)],
        out_specs=[vmem] * 5,
        scratch_shapes=[
            pltpu.VMEM((flat_rows, LANES), F32),
            pltpu.VMEM((flat_rows, LANES), BF16),
            pltpu.VMEM((flat_rows, LANES), BF16),
            pltpu.VMEM((flat_rows, LANES), BF16),
            pltpu.SemaphoreType.DMA((len(groups), depth)),
            pltpu.SemaphoreType.DMA((len(groups), depth)),
            pltpu.SemaphoreType.DMA((len(groups), depth)),
            pltpu.SemaphoreType.DMA((len(groups), depth)),
            pltpu.VMEM((2, hidden // LANES, LANES), F32),
            pltpu.VMEM((tiles, hidden // LANES, LANES), F32),
            pltpu.VMEM((subs, hidden // LANES, LANES), F32),
            pltpu.SemaphoreType.DMA((tiles - 1,)),
            pltpu.SemaphoreType.DMA((tiles - 1,)),
            pltpu.SemaphoreType.DMA((subs - 1,)),
            pltpu.SemaphoreType.DMA((subs - 1,)),
            pltpu.VMEM((phases, buffer_rows, levels), F32),
            pltpu.VMEM((phases, buffer_rows, levels), F32),
            pltpu.VMEM((phases, 8, levels), F32),
            pltpu.VMEM((phases, fan, 8, levels), F32),
            pltpu.VMEM((phases, 8, levels), F32),
            pltpu.VMEM((phases, subs - 1, 8, levels), F32),
            pltpu.VMEM((rows + 2, wide, levels), F32),
            pltpu.VMEM((rows + 2, wide, levels), F32),
            pltpu.VMEM((wide, levels), F32),
            pltpu.VMEM((cols, levels), F32),
            pltpu.VMEM((cols, levels), F32),
            pltpu.VMEM((8, levels), F32),
            pltpu.VMEM((cols, hidden), F32),
            pltpu.VMEM((STEPS, cols, hidden), BF16),
            pltpu.VMEM((STEPS, cols, hidden), F32),
            pltpu.VMEM((STEPS, cols, in_width), BF16),
            pltpu.VMEM((cols, hidden), BF16),
            pltpu.VMEM((cols, levels), BF16),
            pltpu.SemaphoreType.DMA((phases, 8)),
            pltpu.SemaphoreType.DMA((phases, 8)),
            pltpu.SemaphoreType.DMA((phases, fan)),
            pltpu.SemaphoreType.DMA((phases, fan)),
            pltpu.SemaphoreType.DMA((phases, subs - 1)),
            pltpu.SemaphoreType.DMA((phases, subs - 1)),
        ],
        compiler_params=pltpu.CompilerParams(has_side_effects=True, vmem_limit_bytes=48 * 1024 * 1024),
        name="chain",
    )(initial_state, cotangent, w_in, b_in[None, :], w_out, edge_flips)
    return (final, grad, gw_in, gb[0], gw_out)


def solution(mesh):
    in_specs = (P("tile", None, "sub"), P("tile", None, "sub"), P(), P(), P(), P("tile", None))
    out_specs = (P("tile", None, "sub"), P("tile", None, "sub"), P(), P(), P())
    body = functools.partial(shards, mesh.shape["tile"], mesh.shape["sub"])
    return jax.shard_map(body, mesh=mesh, in_specs=in_specs, out_specs=out_specs, check_vma=False)
```

```python
import functools

import jax
import jax.numpy as jnp
from jax import lax
from jax.experimental import pallas as pl
from jax.experimental.pallas import tpu as pltpu
from jax.sharding import PartitionSpec as P

STEPS = 4
TILE_ROW = 4
STEP_SIZE = 0.25
LEAD = 8
MESH = pl.DeviceIdType.MESH
F32 = jnp.float32
BF16 = jnp.bfloat16

LANES = 128
DIRECT_LIMIT = 64


def layout(width, rows):
    names = [("N", width), ("S", width), ("W", rows), ("E", rows)]
    names += [(name, 8) for name in ("NW", "NE", "SW", "SE")]
    place, at = {}, 0
    for name, size in names:
        place[name] = (at, size)
        at += size
    return place, at


def reduce_plan(tiles, subs, flat_rows):
    bits = [("sub", 1 << i) for i in range(subs.bit_length() - 1)]
    bits += [("tile", 1 << i) for i in range(tiles.bit_length() - 1)]
    unit = 16 * tiles * subs
    units = -(-flat_rows // unit)
    count = min(3, units)
    groups, at = [], 0
    for g in range(count):
        size = (units // count + (1 if g < units % count else 0)) * unit
        turning = bits[1:4]
        order = bits[:1] + turning[g:] + turning[:g] + bits[4:]
        groups.append((at, size, order))
        at += size
    return groups, at


def dot(a, b, dims, precision=None):
    return lax.dot_general(a, b, (dims, ((), ())), preferred_element_type=F32, precision=precision)


def chain_kernel(
    tiles, subs, rows, width, levels, hidden,
    state_hbm, cot_hbm, w_in_hbm, b_in_hbm, w_out_hbm, flips_ref,
    final_ref, grad_ref, gw_in_ref, gb_ref, gw_out_ref,
    state_ref, cot_ref, w_in_ref, b_in_ref, w_out_ref, load_sem,
    flat, out_half, in_half, whole, red_ssem, red_rsem, gat_ssem, gat_rsem,
    bias_out, bias_tiles, bias_subs, bias_ssem, bias_rsem, side_ssem, side_rsem,
    send, recv, tile_out, tile_in, sub_out, sub_in,
    padded, pad_grad, edge, field, gradient, totals, pre, hid, slope, patch,
    gp16, gt16,
    halo_ssem, halo_rsem, tile_ssem, tile_rsem, sub_ssem, sub_rsem,
):
    place, _ = layout(width, rows)
    cols = rows * width
    inv_total = 1.0 / (tiles * subs * cols)
    me_t, me_s = lax.axis_index("tile"), lax.axis_index("sub")
    first, last = me_s == 0, me_s == subs - 1
    wide = width + 2 * LEAD

    def tile_at(by):
        return lax.rem(me_t + by + 2 * tiles, tiles)

    def north_of(by):
        return (jnp.where(first, tile_at(by - TILE_ROW), tile_at(by)), jnp.where(first, subs - 1, me_s - 1))

    def south_of(by):
        return (jnp.where(last, tile_at(by + TILE_ROW), tile_at(by)), jnp.where(last, 0, me_s + 1))

    targets = {
        "N": north_of(0), "S": south_of(0), "W": (tile_at(-1), me_s), "E": (tile_at(1), me_s),
        "NW": north_of(-1), "NE": north_of(1), "SW": south_of(-1), "SE": south_of(1),
    }

    def halo_copies(p):
        out = []
        for i, (name, (at, size)) in enumerate(place.items()):
            out.append(pltpu.make_async_remote_copy(
                src_ref=send.at[p, pl.ds(at, size)], dst_ref=recv.at[p, pl.ds(at, size)],
                send_sem=halo_ssem.at[p, i], recv_sem=halo_rsem.at[p, i],
                device_id=targets[name], device_id_type=MESH))
        return out

    direct = tiles * subs <= DIRECT_LIMIT
    me = me_t * subs + me_s

    def sum_copies(p):
        out = []
        for d in range(1, tiles * subs if direct else tiles):
            if direct:
                peer = lax.rem(me + d, tiles * subs)
                there = (peer // subs, lax.rem(peer, subs))
            else:
                there = (tile_at(d), me_s)
            out.append(pltpu.make_async_remote_copy(
                src_ref=tile_out.at[p], dst_ref=tile_in.at[p, d - 1],
                send_sem=tile_ssem.at[p, d - 1], recv_sem=tile_rsem.at[p, d - 1],
                device_id=there, device_id_type=MESH))
        return out

    def sub_copies(p):
        return [pltpu.make_async_remote_copy(
            src_ref=sub_out.at[p], dst_ref=sub_in.at[p, d - 1],
            send_sem=sub_ssem.at[p, d - 1], recv_sem=sub_rsem.at[p, d - 1],
            device_id=(me_t, lax.rem(me_s + d, subs)), device_id_type=MESH) for d in range(1, subs)]

    def start_exchange(p):
        for copy in sum_copies(p) + halo_copies(p):
            copy.start()

    def finish_exchange(p):
        for copy in sum_copies(p):
            copy.wait()
        total = tile_out[p]
        for d in range(1, tiles * subs if direct else tiles):
            total = total + tile_in[p, d - 1]
        if not direct:
            sub_out[p] = total
            for copy in sub_copies(p):
                copy.start()
        for copy in halo_copies(p):
            copy.wait()
        if not direct:
            for copy in sub_copies(p):
                copy.wait()
            for d in range(1, subs):
                total = total + sub_in[p, d - 1]
        return total

    at_row = lax.broadcasted_iota(jnp.int32, (wide, wide), 0)
    at_col = lax.broadcasted_iota(jnp.int32, (wide, wide), 1)
    same = (at_row == at_col).astype(F32)
    turned = (at_row + at_col == wide - 1).astype(F32)

    def seam_matrix(flag, here):
        mix = jnp.where(here, flag, 0).astype(F32)
        return turned * mix + same * (1.0 - mix)

    turn_north = seam_matrix(flips_ref[0, 0], first)
    turn_south = seam_matrix(flips_ref[0, 1], last)

    def send_field(p):
        for name, row in (("N", 0), ("S", rows - 1)):
            at = place[name][0]
            line = field[row * width:(row + 1) * width]
            send[p, at:at + width] = line
            for side, cell in (("W", 0), ("E", width - 1)):
                corner = place[name + side][0]
                send[p, corner:corner + 1] = line[cell:cell + 1]
        for name, cell in (("W", 0), ("E", width - 1)):
            at = place[name][0]
            for r in range(rows):
                send[p, at + r:at + r + 1] = field[r * width + cell:r * width + cell + 1]

    def pad_field(p, shift):
        padded[1:rows + 1, LEAD:LEAD + width, :] = (field[...]).reshape(rows, width, levels)
        for name, cell in (("E", LEAD - 1), ("W", LEAD + width)):
            at = place[name][0]
            for r in range(rows):
                padded[r + 1, cell:cell + 1] = recv[p, at + r:at + r + 1] - shift
        for name, row, turn in (("S", 0, turn_north), ("N", rows + 1, turn_south)):
            at = place[name][0]
            edge[LEAD:LEAD + width] = recv[p, at:at + width] - shift
            for side, cell in (("E", LEAD - 1), ("W", LEAD + width)):
                corner = place[name + side][0]
                edge[cell:cell + 1] = recv[p, corner:corner + 1] - shift
            padded[row] = dot(turn.astype(BF16), edge[...].astype(BF16), ((1,), (0,)))

    pairs = ((state_hbm, state_ref), (cot_hbm, cot_ref), (b_in_hbm, b_in_ref),
             (w_out_hbm, w_out_ref), (w_in_hbm, w_in_ref))
    loads = [pltpu.make_async_copy(a, b, load_sem.at[i]) for i, (a, b) in enumerate(pairs)]
    for load in loads:
        load.start()
    send[...] = jnp.zeros_like(send)
    tile_out[...] = jnp.zeros_like(tile_out)
    edge[...] = jnp.zeros_like(edge)
    loads[0].wait()
    loads[1].wait()
    field[...] = state_ref[0].T
    gradient[...] = cot_ref[0].T
    send_field(0)
    tile_out[0, 1:2] = jnp.sum(gradient[...], axis=0, keepdims=True)
    start_exchange(0)
    gw_in_ref[...] = jnp.zeros_like(gw_in_ref)
    gb_ref[...] = jnp.zeros_like(gb_ref)
    gw_out_ref[...] = jnp.zeros_like(gw_out_ref)
    padded[...] = jnp.zeros_like(padded)

    for load in loads[2:]:
        load.wait()

    def forward(k, carry):
        total = finish_exchange(k)
        shift = total[0:1] * (STEP_SIZE * inv_total)
        field[...] = field[...] - shift

        @pl.when(k == 0)
        def _():
            totals[...] = total

        pad_field(k, shift)
        for a in range(3):
            for b in range(3):
                o = 3 * a + b
                piece = padded[a:a + rows, LEAD - 1 + b:LEAD - 1 + b + width, :]
                patch[k, :, o * levels:(o + 1) * levels] = piece.reshape(cols, levels).astype(BF16)
        act = dot(patch[k], w_in_ref[...], ((1,), (0,))) + b_in_ref[...]
        pre[...] = act
        low = (act * jax.nn.sigmoid(act)).astype(BF16)
        hid[k] = low
        tendency = dot(low, w_out_ref[...], ((1,), (1,)))
        field[...] = field[...] + STEP_SIZE * tendency
        tile_out[k + 1, 0:1] = jnp.sum(tendency, axis=0, keepdims=True)

        @pl.when(k < STEPS - 1)
        def _():
            send_field(k + 1)
            start_exchange(k + 1)

        value = pre[...]
        sig = jax.nn.sigmoid(value)
        slope[k] = sig * (1.0 + value * (1.0 - sig))
        return carry

    lax.fori_loop(0, STEPS, forward, 0)

    def backward(j, carry):
        k = STEPS - 1 - j
        p = STEPS + j
        level_grad = totals[1:2] * (STEP_SIZE * inv_total)
        low_gt = (STEP_SIZE * gradient[...] - level_grad).astype(BF16)
        gt16[...] = low_gt
        gh = dot(low_gt, w_out_ref[...], ((1,), (0,)))
        gp = gh * slope[k]
        pre[...] = gp
        low = gp.astype(BF16)
        gp16[...] = low
        gi = dot(low, w_in_ref[...], ((1,), (1,)))
        pad_grad[...] = jnp.zeros_like(pad_grad)
        for a in range(3):
            for b in range(3):
                o = 3 * a + b
                piece = gi[:, o * levels:(o + 1) * levels].reshape(rows, width, levels)
                pad_grad[a:a + rows, LEAD - 1 + b:LEAD - 1 + b + width, :] += piece
        gi_sum = jnp.sum(gi, axis=0, keepdims=True)
        part = gi_sum[:, 0:levels]
        for o in range(1, 9):
            part = part + gi_sum[:, o * levels:(o + 1) * levels]
        tile_out[p, 1:2] = part
        for name, row, turn in (("N", 0, turn_north), ("S", rows + 1, turn_south)):
            at = place[name][0]
            edge[...] = dot(turn, pad_grad[row], ((1,), (0,)), lax.Precision.HIGHEST)
            send[p, at:at + width] = edge[LEAD:LEAD + width]
            for side, cell in (("W", LEAD - 1), ("E", LEAD + width)):
                corner = place[name + side][0]
                send[p, corner:corner + 1] = edge[cell:cell + 1]
        for name, cell in (("W", LEAD - 1), ("E", LEAD + width)):
            at = place[name][0]
            for r in range(rows):
                send[p, at + r:at + r + 1] = pad_grad[r + 1, cell:cell + 1]
        start_exchange(p)
        gradient[...] += pad_grad[1:rows + 1, LEAD:LEAD + width, :].reshape(cols, levels)
        gw_in_ref[...] += dot(patch[k], gp16[...], ((0,), (0,)))
        gw_out_ref[...] += dot(gt16[...], hid[k], ((0,), (0,)))
        gb_ref[...] += jnp.sum(pre[...], axis=0, keepdims=True)
        total = finish_exchange(p)

        @pl.when(j == 0)
        def _():
            field[...] = field[...] - total[0:1] * (STEP_SIZE * inv_total)

        totals[1:2] = totals[1:2] + total[1:2]
        for name, row in (("N", rows - 1), ("S", 0)):
            at = place[name][0]
            gradient[row * width:(row + 1) * width] += recv[p, at:at + width]
            for side, cell in (("W", width - 1), ("E", 0)):
                corner = place[name + side][0]
                gradient[row * width + cell:row * width + cell + 1] += recv[p, corner:corner + 1]
        for name, cell in (("W", width - 1), ("E", 0)):
            at = place[name][0]
            for r in range(rows):
                gradient[r * width + cell:r * width + cell + 1] += recv[p, at + r:at + r + 1]
        return carry

    lax.fori_loop(0, STEPS, backward, 0)

    in_width = gw_in_ref.shape[0]
    stride = in_width + levels
    for c in range(hidden // LANES):
        bias_out[0, c:c + 1] = gb_ref[:, c * LANES:(c + 1) * LANES]
    bias_tiles[me_t] = bias_out[0]

    def bias_tile_copies():
        return [pltpu.make_async_remote_copy(
            src_ref=bias_out.at[0], dst_ref=bias_tiles.at[me_t],
            send_sem=bias_ssem.at[d - 1], recv_sem=bias_rsem.at[d - 1],
            device_id=(tile_at(d), me_s), device_id_type=MESH) for d in range(1, tiles)]

    def bias_sub_copies():
        return [pltpu.make_async_remote_copy(
            src_ref=bias_out.at[1], dst_ref=bias_subs.at[me_s],
            send_sem=side_ssem.at[d - 1], recv_sem=side_rsem.at[d - 1],
            device_id=(me_t, lax.rem(me_s + d, subs)), device_id_type=MESH) for d in range(1, subs)]

    for copy in bias_tile_copies():
        copy.start()
    groups, flat_rows = reduce_plan(tiles, subs, stride * (hidden // LANES))
    for c in range(hidden // LANES):
        at, lanes = c * stride, slice(c * LANES, (c + 1) * LANES)
        flat[at:at + in_width] = gw_in_ref[:, lanes]
        flat[at + in_width:at + in_width + levels] = gw_out_ref[:, lanes]
    used = stride * (hidden // LANES)
    if flat_rows > used:
        flat[used:flat_rows] = jnp.zeros((flat_rows - used, LANES), F32)

    def bit_of(axis, step):
        index = me_t if axis == "tile" else me_s
        return lax.rem(index // step, 2)

    def peer_of(axis, step):
        if axis == "tile":
            return (me_t + step * (1 - 2 * bit_of(axis, step)), me_s)
        return (me_t, me_s + step * (1 - 2 * bit_of(axis, step)))

    def bases(group):
        start, size, order = group
        out, base = [], start
        for axis, step in order:
            out.append((base, size // 2))
            size = size // 2
            base = base + bit_of(axis, step) * size
        return out, base, size

    depth = len(groups[0][2])

    def reduce_copy(g, i):
        start, size, order = groups[g]
        half = size >> (i + 1)
        at = start + size - (size >> i)
        return pltpu.make_async_remote_copy(
            src_ref=out_half.at[pl.ds(at, half)], dst_ref=in_half.at[pl.ds(at, half)],
            send_sem=red_ssem.at[g, i], recv_sem=red_rsem.at[g, i],
            device_id=peer_of(*order[i]), device_id_type=MESH)

    def gather_copy(g, i):
        start, size, order = groups[g]
        part = size >> (i + 1)
        base = bases(groups[g])[0][i][0] + bit_of(*order[i]) * part
        rows_here = pl.ds(pl.multiple_of(base, 16), part)
        return pltpu.make_async_remote_copy(
            src_ref=whole.at[rows_here], dst_ref=whole.at[rows_here],
            send_sem=gat_ssem.at[g, i], recv_sem=gat_rsem.at[g, i],
            device_id=peer_of(*order[i]), device_id_type=MESH)

    for i in range(depth + 1):
        for g, (start, size, order) in enumerate(groups):
            levels_of = bases((start, size, order))
            if i > 0:
                reduce_copy(g, i - 1).wait()
                base, half = levels_of[0][i - 1]
                at = start + size - (size >> (i - 1))
                kept = pl.ds(pl.multiple_of(base + bit_of(*order[i - 1]) * half, 16), half)
                flat[kept] = flat[kept] + in_half[at:at + half].astype(F32)
            if i < depth:
                base, half = levels_of[0][i]
                at = start + size - (size >> i)
                away = pl.ds(pl.multiple_of(base + (1 - bit_of(*order[i])) * half, 16), half)
                out_half[at:at + half] = flat[away].astype(BF16)
                reduce_copy(g, i).start()
            else:
                own = pl.ds(pl.multiple_of(levels_of[1], 16), levels_of[2])
                whole[own] = flat[own].astype(BF16)
                gather_copy(g, depth - 1).start()
    for copy in bias_tile_copies():
        copy.wait()
    bias = bias_tiles[0]
    for d in range(1, tiles):
        bias = bias + bias_tiles[d]
    bias_out[1] = bias
    bias_subs[me_s] = bias
    for copy in bias_sub_copies():
        copy.start()
    for i in reversed(range(depth)):
        for g in range(len(groups)):
            gather_copy(g, i).wait()
            if i > 0:
                gather_copy(g, i - 1).start()
    for copy in bias_sub_copies():
        copy.wait()
    bias = bias_subs[0]
    for d in range(1, subs):
        bias = bias + bias_subs[d]
    for c in range(hidden // LANES):
        at, lanes = c * stride, slice(c * LANES, (c + 1) * LANES)
        gw_in_ref[:, lanes] = whole[at:at + in_width].astype(F32)
        gw_out_ref[:, lanes] = whole[at + in_width:at + in_width + levels].astype(F32)
        gb_ref[:, lanes] = bias[c:c + 1]
    final_ref[0] = field[...].T
    grad_ref[0] = gradient[...].T


def shards(tiles, subs, initial_state, cotangent, w_in, b_in, w_out, edge_flips):
    _, levels, cols = initial_state.shape
    in_width, hidden = w_in.shape
    side = 1
    while side * side < cols * subs:
        side += 1
    rows, width = side // subs, side
    _, buffer_rows = layout(width, rows)
    phases = 2 * STEPS
    groups, flat_rows = reduce_plan(tiles, subs, (in_width + levels) * (hidden // LANES))
    depth = len(groups[0][2])
    fan = tiles * subs - 1 if tiles * subs <= DIRECT_LIMIT else tiles - 1
    wide = width + 2 * LEAD
    vmem = pl.BlockSpec(memory_space=pltpu.VMEM)
    final, grad, gw_in, gb, gw_out = pl.pallas_call(
        functools.partial(chain_kernel, tiles, subs, rows, width, levels, hidden),
        out_shape=(
            jax.ShapeDtypeStruct(initial_state.shape, F32),
            jax.ShapeDtypeStruct(initial_state.shape, F32),
            jax.ShapeDtypeStruct((in_width, hidden), F32),
            jax.ShapeDtypeStruct((1, hidden), F32),
            jax.ShapeDtypeStruct((levels, hidden), F32),
        ),
        in_specs=[pl.BlockSpec(memory_space=pltpu.HBM)] * 5 + [pl.BlockSpec(memory_space=pltpu.SMEM)],
        out_specs=[vmem] * 5,
        scratch_shapes=[
            pltpu.VMEM(initial_state.shape, F32),
            pltpu.VMEM(cotangent.shape, F32),
            pltpu.VMEM(w_in.shape, BF16),
            pltpu.VMEM((1, hidden), F32),
            pltpu.VMEM(w_out.shape, BF16),
            pltpu.SemaphoreType.DMA((5,)),
            pltpu.VMEM((flat_rows, LANES), F32),
            pltpu.VMEM((flat_rows, LANES), BF16),
            pltpu.VMEM((flat_rows, LANES), BF16),
            pltpu.VMEM((flat_rows, LANES), BF16),
            pltpu.SemaphoreType.DMA((len(groups), depth)),
            pltpu.SemaphoreType.DMA((len(groups), depth)),
            pltpu.SemaphoreType.DMA((len(groups), depth)),
            pltpu.SemaphoreType.DMA((len(groups), depth)),
            pltpu.VMEM((2, hidden // LANES, LANES), F32),
            pltpu.VMEM((tiles, hidden // LANES, LANES), F32),
            pltpu.VMEM((subs, hidden // LANES, LANES), F32),
            pltpu.SemaphoreType.DMA((tiles - 1,)),
            pltpu.SemaphoreType.DMA((tiles - 1,)),
            pltpu.SemaphoreType.DMA((subs - 1,)),
            pltpu.SemaphoreType.DMA((subs - 1,)),
            pltpu.VMEM((phases, buffer_rows, levels), F32),
            pltpu.VMEM((phases, buffer_rows, levels), F32),
            pltpu.VMEM((phases, 8, levels), F32),
            pltpu.VMEM((phases, fan, 8, levels), F32),
            pltpu.VMEM((phases, 8, levels), F32),
            pltpu.VMEM((phases, subs - 1, 8, levels), F32),
            pltpu.VMEM((rows + 2, wide, levels), F32),
            pltpu.VMEM((rows + 2, wide, levels), F32),
            pltpu.VMEM((wide, levels), F32),
            pltpu.VMEM((cols, levels), F32),
            pltpu.VMEM((cols, levels), F32),
            pltpu.VMEM((8, levels), F32),
            pltpu.VMEM((cols, hidden), F32),
            pltpu.VMEM((STEPS, cols, hidden), BF16),
            pltpu.VMEM((STEPS, cols, hidden), F32),
            pltpu.VMEM((STEPS, cols, in_width), BF16),
            pltpu.VMEM((cols, hidden), BF16),
            pltpu.VMEM((cols, levels), BF16),
            pltpu.SemaphoreType.DMA((phases, 8)),
            pltpu.SemaphoreType.DMA((phases, 8)),
            pltpu.SemaphoreType.DMA((phases, fan)),
            pltpu.SemaphoreType.DMA((phases, fan)),
            pltpu.SemaphoreType.DMA((phases, subs - 1)),
            pltpu.SemaphoreType.DMA((phases, subs - 1)),
        ],
        compiler_params=pltpu.CompilerParams(has_side_effects=True, vmem_limit_bytes=48 * 1024 * 1024),
        name="chain",
    )(initial_state, cotangent, w_in, b_in[None, :], w_out, edge_flips)
    return (final, grad, gw_in, gb[0], gw_out)


def solution(mesh):
    in_specs = (P("tile", None, "sub"), P("tile", None, "sub"), P(), P(), P(), P("tile", None))
    out_specs = (P("tile", None, "sub"), P("tile", None, "sub"), P(), P(), P())
    body = functools.partial(shards, mesh.shape["tile"], mesh.shape["sub"])
    return jax.shard_map(body, mesh=mesh, in_specs=in_specs, out_specs=out_specs, check_vma=False)
```
